8 devices in a mesh: dp: 1 (over z), tp: 2 (over y), cp: 4 (over x, core).
Axes of the slice: x: 2, y: 2, z: 1, core: 2. Of those that a mesh axis runs over, the one named last changes fastest.
Arguments:
- x_chunk: bfloat16 [32, 64, 5120], P('dp', 'cp')
- w_query: bfloat16 [5120, 5120], P(None, 'tp')
- w_key: bfloat16 [5120, 1024], P(None, 'tp')
- w_value: bfloat16 [5120, 1024], P(None, 'tp')
- w_out: bfloat16 [5120, 5120], P('tp')
- q_gain: bfloat16 [5120], P('tp')
- k_gain: bfloat16 [1024], P('tp')
- post_gain: bfloat16 [5120], replicated
- cache_k: bfloat16 [32, 4096, 8, 128], P('dp', 'cp', 'tp')
- cache_v: bfloat16 [32, 4096, 8, 128], P('dp', 'cp', 'tp')
- prefix_len: int32 [32], P('dp')
Outputs:
- output 1: bfloat16 [32, 64, 5120], P('dp', 'cp')
- output 2: bfloat16 [32, 64, 8, 128], P('dp', 'cp', 'tp')
- output 3: bfloat16 [32, 64, 8, 128], P('dp', 'cp', 'tp')
All inputs are finite; a program needn't handle non-finite values.
Results may differ from the reference program's by a relative error of at most 0.00717723.
Values are sent between devices in bfloat16 or wider.
A program may use at most 1 GiB of HBM per device.

```python
import jax
import jax.numpy as jnp
from jax import lax

BATCH_ROWS = 32
CHUNK_LEN = 64
CACHE_LEN = 4096
MODEL_DIM = 5120
Q_HEADS = 40
KV_HEADS = 8
HEAD_DIM = 128
QUERY_BLOCK = min(CHUNK_LEN, 16)
ROPE_BASE = 500000.0
NORM_EPS = 1e-6


def head_scales(rng_key, n_heads, trend_slope):
    trend_pos = jnp.arange(n_heads, dtype=jnp.float32) * (2.0 / max(n_heads - 1, 1)) - 1.0
    noise_val = jax.random.normal(rng_key, (n_heads,), jnp.float32)
    return jnp.exp(trend_slope * trend_pos + 0.2 * noise_val)


def draw_prefix(rng_key):
    key_order, key_len = jax.random.split(rng_key)
    row_order = jax.random.permutation(key_order, BATCH_ROWS)
    lengths = jax.random.randint(key_len, (BATCH_ROWS,), CACHE_LEN // 2, CACHE_LEN + 1)
    lengths = jnp.where(row_order == 0, CACHE_LEN, jnp.where(row_order == 1, CACHE_LEN // 2, lengths))
    return lengths.astype(jnp.int32)


def setup_inputs(seed: int = 0, part: int = 0) -> dict:
    shared_keys = jax.random.split(jax.random.key(seed), 9)
    own_keys = jax.random.split(jax.random.fold_in(jax.random.key(seed + 1), part), 4)
    q_width = Q_HEADS * HEAD_DIM
    kv_width = KV_HEADS * HEAD_DIM
    q_cols = jnp.repeat(head_scales(shared_keys[0], Q_HEADS, 0.5), HEAD_DIM)
    k_cols = jnp.repeat(head_scales(shared_keys[1], KV_HEADS, 0.5), HEAD_DIM)
    w_query = jax.random.normal(shared_keys[2], (MODEL_DIM, q_width), jnp.float32) * (MODEL_DIM ** -0.5) * q_cols[None, :]
    w_key = jax.random.normal(shared_keys[3], (MODEL_DIM, kv_width), jnp.float32) * (MODEL_DIM ** -0.5) * k_cols[None, :]
    w_value = jax.random.normal(shared_keys[4], (MODEL_DIM, kv_width), jnp.float32) * (MODEL_DIM ** -0.5)
    w_out = jax.random.normal(shared_keys[5], (q_width, MODEL_DIM), jnp.float32) * (q_width ** -0.5)
    q_gain = 1.0 + 0.25 * jax.random.normal(shared_keys[6], (q_width,), jnp.float32)
    k_gain = 1.0 + 0.25 * jax.random.normal(shared_keys[7], (kv_width,), jnp.float32)
    post_gain = 1.0 + 0.3 * jax.random.normal(shared_keys[8], (MODEL_DIM,), jnp.float32)
    prefix_len = draw_prefix(own_keys[0])
    x_chunk = jax.random.normal(own_keys[1], (BATCH_ROWS, CHUNK_LEN, MODEL_DIM), jnp.float32)
    stale_mask = jnp.arange(CACHE_LEN)[None, :] >= prefix_len[:, None]
    slot_scale = jnp.where(stale_mask, 3.0, 1.0)[:, :, None, None]
    cache_k = 0.8 * jax.random.normal(own_keys[2], (BATCH_ROWS, CACHE_LEN, KV_HEADS, HEAD_DIM), jnp.float32) * slot_scale
    cache_v = jax.random.normal(own_keys[3], (BATCH_ROWS, CACHE_LEN, KV_HEADS, HEAD_DIM), jnp.float32) * slot_scale
    return {
        'x_chunk': x_chunk.astype(jnp.bfloat16),
        'w_query': w_query.astype(jnp.bfloat16),
        'w_key': w_key.astype(jnp.bfloat16),
        'w_value': w_value.astype(jnp.bfloat16),
        'w_out': w_out.astype(jnp.bfloat16),
        'q_gain': q_gain.astype(jnp.bfloat16),
        'k_gain': k_gain.astype(jnp.bfloat16),
        'post_gain': post_gain.astype(jnp.bfloat16),
        'cache_k': cache_k.astype(jnp.bfloat16),
        'cache_v': cache_v.astype(jnp.bfloat16),
        'prefix_len': prefix_len,
    }


def rms_norm(raw_vals, gain_vec):
    mean_sq = jnp.mean(raw_vals * raw_vals, axis=-1, keepdims=True)
    return raw_vals * lax.rsqrt(mean_sq + NORM_EPS) * gain_vec.astype(jnp.float32)


def rope_apply(head_vals, positions):
    half_dim = HEAD_DIM // 2
    inv_freq = ROPE_BASE ** (-(jnp.arange(half_dim, dtype=jnp.float32) * 2.0 / HEAD_DIM))
    angles = positions.astype(jnp.float32)[..., None] * inv_freq
    cos_tab = jnp.cos(angles)[..., None, :]
    sin_tab = jnp.sin(angles)[..., None, :]
    first_half = head_vals[..., :half_dim]
    second_half = head_vals[..., half_dim:]
    return jnp.concatenate([first_half * cos_tab - second_half * sin_tab, second_half * cos_tab + first_half * sin_tab], axis=-1)


def reference(x_chunk, w_query, w_key, w_value, w_out, q_gain, k_gain, post_gain, cache_k, cache_v, prefix_len):
    groups = Q_HEADS // KV_HEADS
    tokens = x_chunk.reshape(BATCH_ROWS * CHUNK_LEN, MODEL_DIM)
    q_raw = jnp.dot(tokens, w_query, preferred_element_type=jnp.float32)
    k_raw = jnp.dot(tokens, w_key, preferred_element_type=jnp.float32)
    v_raw = jnp.dot(tokens, w_value, preferred_element_type=jnp.float32)
    positions = prefix_len[:, None] + jnp.arange(CHUNK_LEN, dtype=jnp.int32)[None, :]
    q_rot = rope_apply(rms_norm(q_raw, q_gain).reshape(BATCH_ROWS, CHUNK_LEN, Q_HEADS, HEAD_DIM), positions)
    k_rot = rope_apply(rms_norm(k_raw, k_gain).reshape(BATCH_ROWS, CHUNK_LEN, KV_HEADS, HEAD_DIM), positions)
    q_new = q_rot.astype(jnp.bfloat16).reshape(BATCH_ROWS, CHUNK_LEN, KV_HEADS, groups, HEAD_DIM)
    chunk_k = k_rot.astype(jnp.bfloat16)
    chunk_v = v_raw.astype(jnp.bfloat16).reshape(BATCH_ROWS, CHUNK_LEN, KV_HEADS, HEAD_DIM)
    key_index = jnp.arange(CACHE_LEN + CHUNK_LEN)
    score_scale = HEAD_DIM ** -0.5

    def row_attention(row_in):
        q_row, k_row, v_row, ck_row, cv_row, valid_len = row_in
        all_keys = jnp.concatenate([ck_row, k_row], axis=0).astype(jnp.float32)
        all_values = jnp.concatenate([cv_row, v_row], axis=0).astype(jnp.float32)
        q_blocks = q_row.reshape(CHUNK_LEN // QUERY_BLOCK, QUERY_BLOCK, KV_HEADS, groups, HEAD_DIM).astype(jnp.float32)

        def block_attention(block_in):
            q_blk, block_id = block_in
            q_index = block_id * QUERY_BLOCK + jnp.arange(QUERY_BLOCK)
            allowed = jnp.where(key_index[None, :] < CACHE_LEN, key_index[None, :] < valid_len, key_index[None, :] - CACHE_LEN <= q_index[:, None])
            scores = jnp.einsum('qkgd,tkd->qkgt', q_blk, all_keys) * score_scale
            scores = jnp.where(allowed[:, None, None, :], scores, -jnp.inf)
            probs_f = jax.nn.softmax(scores, axis=-1)
            return jnp.einsum('qkgt,tkd->qkgd', probs_f, all_values)

        blocks = lax.map(block_attention, (q_blocks, jnp.arange(CHUNK_LEN // QUERY_BLOCK)))
        return blocks.reshape(CHUNK_LEN, Q_HEADS * HEAD_DIM)

    attn_out = lax.map(row_attention, (q_new, chunk_k, chunk_v, cache_k, cache_v, prefix_len))
    attn_out = attn_out.astype(jnp.bfloat16).reshape(BATCH_ROWS * CHUNK_LEN, Q_HEADS * HEAD_DIM)
    mixed_sum = jnp.dot(attn_out, w_out, preferred_element_type=jnp.float32)
    result = x_chunk.astype(jnp.float32) + rms_norm(mixed_sum, post_gain).reshape(BATCH_ROWS, CHUNK_LEN, MODEL_DIM)
    return result.astype(jnp.bfloat16), chunk_k, chunk_v
```

```python
import functools
import math

import jax
import jax.numpy as jnp
from jax import lax
from jax.experimental import pallas as pl
from jax.experimental.pallas import tpu as pltpu
from jax.sharding import PartitionSpec as P

NORM_EPS = 1e-6
ROPE_BASE = 500000.0
MASK_VALUE = -1e30
N_GROUPS = 4


def rope_apply(head_vals, positions):
    head_dim = head_vals.shape[-1]
    half_dim = head_dim // 2
    inv_freq = ROPE_BASE ** (-(jnp.arange(half_dim, dtype=jnp.float32) * 2.0 / head_dim))
    angles = positions.astype(jnp.float32)[..., None] * inv_freq
    cos_tab = jnp.cos(angles)[..., None, :]
    sin_tab = jnp.sin(angles)[..., None, :]
    first_half = head_vals[..., :half_dim]
    second_half = head_vals[..., half_dim:]
    return jnp.concatenate([first_half * cos_tab - second_half * sin_tab, second_half * cos_tab + first_half * sin_tab], axis=-1)


def attention_kernel(dims, prefix_ref, meta_ref, q_own, q_x, q_core, q_diag, k_ref, v_ref, kn_ref, vn_ref, stay_ref, send_ref, kf, vf, kc, vc):
    first_row, kv, groups, chunk, slots, hd = dims
    b = pl.program_id(0)
    cp = meta_ref[0]
    rows = groups * chunk
    qn = 4 * rows
    scale2 = hd ** -0.5 * math.log2(math.e)
    valid = prefix_ref[first_row + b] - cp * slots
    kf[...] = k_ref[0].astype(jnp.float32)
    vf[...] = v_ref[0].astype(jnp.float32)

    @pl.when(b == 0)
    def _():
        kc[...] = jnp.zeros_like(kc)
        vc[...] = jnp.zeros_like(vc)

    slot_ok = lax.broadcasted_iota(jnp.int32, (1, slots), 1) < valid
    row_id = lax.broadcasted_iota(jnp.int32, (qn, hd), 0)
    lane_id = lax.broadcasted_iota(jnp.int32, (qn, hd), 1)
    seg = row_id // rows
    owner = jnp.where(seg == 0, cp, jnp.where(seg == 1, cp ^ 2, jnp.where(seg == 2, cp ^ 1, cp ^ 3)))
    chunk_ok = (lane_id < chunk) & (cp * chunk + lane_id <= owner * chunk + row_id % chunk)
    for n in range(kv):
        lo = n * rows
        q = jnp.concatenate([r[0, lo:lo + rows] for r in (q_own, q_x, q_core, q_diag)], axis=0)
        kh = kf[pl.ds(n, slots, stride=kv), :].astype(jnp.bfloat16)
        vh = vf[pl.ds(n, slots, stride=kv), :].astype(jnp.bfloat16)
        kc[n, :chunk] = kn_ref[0, n]
        vc[n, :chunk] = vn_ref[0, n]
        nt = (((1,), (1,)), ((), ()))
        s_cache = jnp.where(slot_ok, lax.dot_general(q, kh, nt, preferred_element_type=jnp.float32), MASK_VALUE)
        s_chunk = jnp.where(chunk_ok, lax.dot_general(q, kc[n], nt, preferred_element_type=jnp.float32), MASK_VALUE)
        top = jnp.maximum(jnp.max(s_cache, axis=-1, keepdims=True), jnp.max(s_chunk, axis=-1, keepdims=True))
        off = top * scale2
        p_cache = jnp.exp2(s_cache * scale2 - off)
        p_chunk = jnp.exp2(s_chunk * scale2 - off)
        den = jnp.sum(p_cache, axis=-1, keepdims=True) + jnp.sum(p_chunk, axis=-1, keepdims=True)
        num = jnp.dot(p_cache.astype(jnp.bfloat16), vh, preferred_element_type=jnp.float32)
        num = num + jnp.dot(p_chunk.astype(jnp.bfloat16), vc[n], preferred_element_type=jnp.float32)
        out = num / den
        lse = jnp.broadcast_to(off + jnp.log2(den), (qn, hd))
        for i, ref in enumerate((stay_ref.at[0], stay_ref.at[1], send_ref.at[0], send_ref.at[1])):
            part = slice(i * rows, (i + 1) * rows)
            ref[0, lo:lo + rows] = out[part]
            wide = jnp.concatenate([lse[part], jnp.zeros((hd - rows, hd), jnp.float32)], axis=0).T
            ref[0, kv * rows + n:kv * rows + n + 1] = wide[0:1]


def spread(row, rows):
    return jnp.broadcast_to(row, (row.shape[-1], row.shape[-1])).T[:rows]


def merge_send_kernel(kv, rows, a_ref, b_ref, o_ref):
    base = kv * rows
    la, lb = a_ref[0, 0, base:base + kv], b_ref[0, 0, base:base + kv]
    top = jnp.maximum(la, lb)
    wa, wb = jnp.exp2(la - top), jnp.exp2(lb - top)
    total = wa + wb
    o_ref[0, base:base + kv] = top + jnp.log2(total)
    o_ref[0, base + kv:] = jnp.zeros_like(o_ref[0, base + kv:])
    wa, wb = wa / total, wb / total
    for n in range(kv):
        part = slice(n * rows, (n + 1) * rows)
        o_ref[0, part] = a_ref[0, 0, part] * spread(wa[n:n + 1], rows) + b_ref[0, 0, part] * spread(wb[n:n + 1], rows)


def out_proj_kernel(dims, meta_ref, a_ref, b_ref, c_ref, w_ref, keep_ref, send_ref, o_buf):
    kv, groups, chunk, hd = dims
    rows = groups * chunk
    base = kv * rows
    n_rows = a_ref.shape[1]

    @pl.when(pl.program_id(0) == 0)
    def _():
        def one(i, carry):
            la, lb, lc = a_ref[0, i, base:base + kv], b_ref[0, i, base:base + kv], c_ref[i, base:base + kv]
            top = jnp.maximum(jnp.maximum(la, lb), lc)
            wa, wb, wc = jnp.exp2(la - top), jnp.exp2(lb - top), jnp.exp2(lc - top)
            total = wa + wb + wc
            wa, wb, wc = wa / total, wb / total, wc / total
            for n in range(kv):
                part = slice(n * rows, (n + 1) * rows)
                o = a_ref[0, i, part] * spread(wa[n:n + 1], rows) + b_ref[0, i, part] * spread(wb[n:n + 1], rows) + c_ref[i, part] * spread(wc[n:n + 1], rows)
                o = o.astype(jnp.bfloat16)
                for g in range(groups):
                    col = (n * groups + g) * hd
                    o_buf[pl.ds(pl.multiple_of(i * chunk, chunk), chunk), col:col + hd] = o[g * chunk:(g + 1) * chunk]
            return carry

        lax.fori_loop(0, n_rows, one, 0)

    res = jnp.dot(o_buf[...], w_ref[...], preferred_element_type=jnp.float32)
    half = res.shape[0] // 2
    first = meta_ref[1] == 0
    keep_ref[...] = jnp.where(first, res[:half], res[half:])
    send_ref[...] = jnp.where(first, res[half:], res[:half])


def finish_kernel(meta_ref, a_ref, b_ref, x_ref, g_ref, o_ref):
    n, t, d = x_ref.shape
    a = a_ref[...] + b_ref[...]
    inv = lax.rsqrt(jnp.mean(a * a, axis=-1, keepdims=True) + NORM_EPS)
    y = x_ref[...].reshape(n * t, d).astype(jnp.float32) + a * inv * g_ref[...].astype(jnp.float32)
    o_ref[...] = y.astype(o_ref.dtype).reshape(n, t, d)


def solution(mesh):
    cp_size = mesh.shape['cp']
    tp_size = mesh.shape['tp']

    def local_step(x_chunk, w_query, w_key, w_value, w_out, q_gain, k_gain, post_gain, cache_k, cache_v, prefix_len):
        batch_rows, chunk, model_dim = x_chunk.shape
        slots = cache_k.shape[1]
        kv = cache_k.shape[2]
        hd = cache_k.shape[3]
        heads = w_query.shape[1] // hd
        groups = heads // kv
        rows = groups * chunk
        cp_index = lax.axis_index('cp')
        tp_index = lax.axis_index('tp')
        meta = jnp.stack([cp_index, tp_index]).astype(jnp.int32)
        tokens = x_chunk.reshape(batch_rows * chunk, model_dim)
        q_raw = jnp.dot(tokens, w_query, preferred_element_type=jnp.float32)
        k_raw = jnp.dot(tokens, w_key, preferred_element_type=jnp.float32)
        v_raw = jnp.dot(tokens, w_value, preferred_element_type=jnp.float32)
        tp_flip = [(0, 1), (1, 0)]
        x_flip = [(i, i ^ 2) for i in range(cp_size)]
        core_flip = [(i, i ^ 1) for i in range(cp_size)]
        square_sums = jnp.stack([jnp.sum(q_raw * q_raw, axis=-1), jnp.sum(k_raw * k_raw, axis=-1)])
        square_sums = square_sums + lax.ppermute(square_sums, 'tp', tp_flip)
        q_inv = lax.rsqrt(square_sums[0] / (w_query.shape[1] * tp_size) + NORM_EPS)
        k_inv = lax.rsqrt(square_sums[1] / (w_key.shape[1] * tp_size) + NORM_EPS)
        q_norm = (q_raw * q_inv[:, None] * q_gain.astype(jnp.float32)).reshape(batch_rows, chunk, heads, hd)
        k_norm = (k_raw * k_inv[:, None] * k_gain.astype(jnp.float32)).reshape(batch_rows, chunk, kv, hd)
        positions = prefix_len[:, None] + cp_index * chunk + jnp.arange(chunk, dtype=jnp.int32)[None, :]
        q_new = rope_apply(q_norm, positions).astype(jnp.bfloat16)
        q_new = q_new.transpose(0, 2, 1, 3).reshape(batch_rows, kv * rows, hd)
        chunk_k = rope_apply(k_norm, positions).astype(jnp.bfloat16)
        chunk_v = v_raw.astype(jnp.bfloat16).reshape(batch_rows, chunk, kv, hd)
        k_new, v_new = chunk_k.transpose(0, 2, 1, 3), chunk_v.transpose(0, 2, 1, 3)
        flat_k = cache_k.reshape(batch_rows, slots * kv, hd)
        flat_v = cache_v.reshape(batch_rows, slots * kv, hd)
        n_rows = batch_rows // N_GROUPS
        tall = kv * rows + 8
        gain = post_gain.reshape(1, model_dim)
        f32 = jnp.float32

        def attend(g, q4):
            first = g * n_rows
            q_spec = pl.BlockSpec((1, kv * rows, hd), lambda i, *_: (i, 0, 0))
            c_spec = pl.BlockSpec((1, slots * kv, hd), lambda i, *_: (first + i, 0, 0))
            n_spec = pl.BlockSpec((1, kv, chunk, hd), lambda i, *_: (first + i, 0, 0, 0))
            o_spec = pl.BlockSpec((2, 1, tall, hd), lambda i, *_: (0, i, 0, 0))
            o_type = jax.ShapeDtypeStruct((2, n_rows, tall, hd), f32)
            return pl.pallas_call(
                functools.partial(attention_kernel, (first, kv, groups, chunk, slots, hd)),
                grid_spec=pltpu.PrefetchScalarGridSpec(
                    num_scalar_prefetch=2, grid=(n_rows,),
                    in_specs=[q_spec] * 4 + [c_spec] * 2 + [n_spec] * 2,
                    out_specs=[o_spec] * 2,
                    scratch_shapes=[pltpu.VMEM((slots * kv, hd), f32)] * 2 + [pltpu.VMEM((kv, hd, hd), jnp.bfloat16)] * 2),
                out_shape=[o_type] * 2,
                cost_estimate=pl.CostEstimate(flops=n_rows * kv * 4 * rows * slots * hd * 4 * 3, bytes_accessed=n_rows * slots * kv * hd * 4, transcendentals=n_rows * kv * 4 * rows * slots),
                compiler_params=pltpu.CompilerParams(vmem_limit_bytes=60 * 2 ** 20),
                name='attend',
            )(prefix_len, meta, *q4, flat_k, flat_v, k_new, v_new)

        def merge_send(stay, got):
            spec = pl.BlockSpec((1, 1, tall, hd), lambda i: (1, i, 0, 0))
            return pl.pallas_call(
                functools.partial(merge_send_kernel, kv, rows),
                grid=(n_rows,), in_specs=[spec] * 2, out_specs=pl.BlockSpec((1, tall, hd), lambda i: (i, 0, 0)),
                out_shape=jax.ShapeDtypeStruct((n_rows, tall, hd), f32),
                cost_estimate=pl.CostEstimate(flops=n_rows * tall * hd * 600, bytes_accessed=n_rows * tall * hd * 12, transcendentals=0),
                name='merge_send',
            )(stay, got)

        def out_proj(stay, got, far):
            tile = 1024
            spec = pl.BlockSpec((1, n_rows, tall, hd), lambda j, *_: (0, 0, 0, 0))
            m = n_rows * chunk
            o_type = jax.ShapeDtypeStruct((m // 2, model_dim), f32)
            return pl.pallas_call(
                functools.partial(out_proj_kernel, (kv, groups, chunk, hd)),
                grid_spec=pltpu.PrefetchScalarGridSpec(
                    num_scalar_prefetch=1, grid=(model_dim // tile,),
                    in_specs=[spec, spec, pl.BlockSpec((n_rows, tall, hd), lambda j, *_: (0, 0, 0)), pl.BlockSpec((heads * hd, tile), lambda j, *_: (0, j))],
                    out_specs=[pl.BlockSpec((m // 2, tile), lambda j, *_: (0, j))] * 2,
                    scratch_shapes=[pltpu.VMEM((m, heads * hd), jnp.bfloat16)]),
                out_shape=[o_type] * 2,
                cost_estimate=pl.CostEstimate(flops=m * heads * hd * model_dim * 4, bytes_accessed=heads * hd * model_dim * 2, transcendentals=0),
                compiler_params=pltpu.CompilerParams(vmem_limit_bytes=60 * 2 ** 20),
                name='out_proj',
            )(meta, stay, got, far, w_out)

        def finish(g, keep, far):
            half = n_rows // 2
            m = half * chunk
            spec = pl.BlockSpec((chunk, model_dim), lambda i, *_: (i, 0))
            return pl.pallas_call(
                finish_kernel,
                grid_spec=pltpu.PrefetchScalarGridSpec(
                    num_scalar_prefetch=1, grid=(half,),
                    in_specs=[spec, spec, pl.BlockSpec((1, chunk, model_dim), lambda i, meta: (g * n_rows + meta[1] * half + i, 0, 0)), pl.BlockSpec((1, model_dim), lambda i, *_: (0, 0))],
                    out_specs=pl.BlockSpec((1, chunk, model_dim), lambda i, *_: (i, 0, 0))),
                out_shape=jax.ShapeDtypeStruct((half, chunk, model_dim), jnp.bfloat16),
                cost_estimate=pl.CostEstimate(flops=m * model_dim * 600, bytes_accessed=m * model_dim * 12, transcendentals=0),
                name='finish',
            )(meta, keep, far, x_chunk, gain)

        mine, theirs = [], []
        for g in range(N_GROUPS):
            q = q_new[g * n_rows:(g + 1) * n_rows]
            q_x = lax.ppermute(q, 'cp', x_flip)
            q_core = lax.ppermute(q, 'cp', core_flip)
            q_diag = lax.ppermute(q_x, 'cp', core_flip)
            stay, send = attend(g, (q, q_x, q_core, q_diag))
            got = lax.ppermute(send, 'cp', core_flip)
            far = lax.ppermute(merge_send(stay, got), 'cp', x_flip)
            keep, give = out_proj(stay, got, far)
            done = finish(g, keep, lax.ppermute(give, 'tp', tp_flip))
            mine.append(done)
            theirs.append(lax.ppermute(done, 'tp', tp_flip))
        even = jnp.concatenate([z for pair in zip(mine, theirs) for z in pair], axis=0)
        odd = jnp.concatenate([z for pair in zip(theirs, mine) for z in pair], axis=0)
        return jnp.where(tp_index == 0, even, odd), chunk_k, chunk_v

    x_spec = P('dp', 'cp', None)
    head_spec = P('dp', 'cp', 'tp', None)
    in_specs = (x_spec, P(None, 'tp'), P(None, 'tp'), P(None, 'tp'), P('tp', None), P('tp'), P('tp'), P(None), head_spec, head_spec, P('dp'))
    out_specs = (x_spec, head_spec, head_spec)
    return jax.shard_map(local_step, mesh=mesh, in_specs=in_specs, out_specs=out_specs, check_vma=False)
```
